8 devices in a mesh: pod: 1 (over z), dp: 2 (over y), sp: 4 (over x, core).
Axes of the slice: x: 2, y: 2, z: 1, core: 2. Of those that a mesh axis runs over, the one named last changes fastest.
Arguments:
- x: bfloat16 [6, 192, 128, 1152], P(('pod', 'dp'), 'sp')
- norm_gain: bfloat16 [2, 2, 1152], replicated
- norm_shift: bfloat16 [2, 2, 1152], replicated
- w_qkv: bfloat16 [2, 3, 1152, 16, 72], replicated
- w_out: bfloat16 [2, 16, 72, 1152], replicated
- w_up: bfloat16 [2, 1152, 4608], replicated
- w_down: bfloat16 [2, 4608, 1152], replicated
Outputs:
- output: bfloat16 [6, 192, 128, 1152], P(('pod', 'dp'), 'sp')
All inputs are finite; a program needn't handle non-finite values.
Results may differ from the reference program's by a relative error of at most 0.0150801.
Values are sent between devices in bfloat16 or wider.
A program may use at most 1 GiB of HBM per device.

```python
import jax
import jax.numpy as jnp
from jax import lax

NUM_VIDEOS = 6
NUM_FRAMES = 192
NUM_PATCHES = 128
MODEL_WIDTH = 1152
NUM_HEADS = 16

HEAD_DIM = MODEL_WIDTH // NUM_HEADS
FF_WIDTH = 4 * MODEL_WIDTH
LN_EPS = 1e-6
QK_GAIN = 1.5


def layer_norm(tokens, gain, shift):
    tok_f = tokens.astype(jnp.float32)
    mean_val = jnp.mean(tok_f, axis=-1, keepdims=True)
    centered = tok_f - mean_val
    var_val = jnp.mean(centered * centered, axis=-1, keepdims=True)
    normed = centered * lax.rsqrt(var_val + LN_EPS)
    return (normed * gain.astype(jnp.float32) + shift.astype(jnp.float32)).astype(jnp.bfloat16)


def seq_block(tokens, gains, shifts, w_qkv, w_out, w_up, w_down):
    normed = layer_norm(tokens, gains[0], shifts[0])
    proj_qkv = jnp.einsum('ld,kdhe->klhe', normed.astype(jnp.float32), w_qkv.astype(jnp.float32)).astype(jnp.bfloat16)
    scores = jnp.einsum('lhe,mhe->hlm', proj_qkv[0].astype(jnp.float32), proj_qkv[1].astype(jnp.float32)) * (HEAD_DIM ** -0.5)
    attn_probs = jax.nn.softmax(scores, axis=-1).astype(jnp.bfloat16)
    mixed = jnp.einsum('hlm,mhe->lhe', attn_probs.astype(jnp.float32), proj_qkv[2].astype(jnp.float32)).astype(jnp.bfloat16)
    attn_proj = jnp.einsum('lhe,hed->ld', mixed.astype(jnp.float32), w_out.astype(jnp.float32)).astype(jnp.bfloat16)
    hidden = (tokens.astype(jnp.float32) + attn_proj.astype(jnp.float32)).astype(jnp.bfloat16)
    normed_mlp = layer_norm(hidden, gains[1], shifts[1])
    up_proj = jnp.dot(normed_mlp, w_up, preferred_element_type=jnp.float32).astype(jnp.bfloat16)
    activated = jax.nn.gelu(up_proj.astype(jnp.float32), approximate=True).astype(jnp.bfloat16)
    down_proj = jnp.dot(activated, w_down, preferred_element_type=jnp.float32).astype(jnp.bfloat16)
    return (hidden.astype(jnp.float32) + down_proj.astype(jnp.float32)).astype(jnp.bfloat16)


def setup_inputs(seed: int = 0, part: int = 0) -> dict:
    base_key = jax.random.key(seed)
    key_list = jax.random.split(base_key, 7)
    data_key = jax.random.fold_in(key_list[0], part)
    key_frame, key_patch, key_noise = jax.random.split(data_key, 3)
    frame_code = jax.random.normal(key_frame, (NUM_VIDEOS, NUM_FRAMES, 1, MODEL_WIDTH), jnp.float32)
    patch_code = jax.random.normal(key_patch, (NUM_VIDEOS, 1, NUM_PATCHES, MODEL_WIDTH), jnp.float32)
    noise_val = jax.random.normal(key_noise, (NUM_VIDEOS, NUM_FRAMES, NUM_PATCHES, MODEL_WIDTH), jnp.float32)
    x = (frame_code + patch_code + 0.5 * noise_val).astype(jnp.bfloat16)
    norm_gain = (1.0 + 0.4 * jax.random.normal(key_list[1], (2, 2, MODEL_WIDTH), jnp.float32)).astype(jnp.bfloat16)
    norm_shift = (0.4 * jax.random.normal(key_list[2], (2, 2, MODEL_WIDTH), jnp.float32)).astype(jnp.bfloat16)
    qkv_gain = jnp.array([QK_GAIN, QK_GAIN, 1.0], jnp.float32).reshape(1, 3, 1, 1, 1)
    w_qkv = (jax.random.normal(key_list[3], (2, 3, MODEL_WIDTH, NUM_HEADS, HEAD_DIM), jnp.float32) * (MODEL_WIDTH ** -0.5) * qkv_gain).astype(jnp.bfloat16)
    w_out = (jax.random.normal(key_list[4], (2, NUM_HEADS, HEAD_DIM, MODEL_WIDTH), jnp.float32) * (MODEL_WIDTH ** -0.5)).astype(jnp.bfloat16)
    w_up = (jax.random.normal(key_list[5], (2, MODEL_WIDTH, FF_WIDTH), jnp.float32) * (MODEL_WIDTH ** -0.5)).astype(jnp.bfloat16)
    w_down = (jax.random.normal(key_list[6], (2, FF_WIDTH, MODEL_WIDTH), jnp.float32) * (FF_WIDTH ** -0.5)).astype(jnp.bfloat16)
    return {'x': x, 'norm_gain': norm_gain, 'norm_shift': norm_shift, 'w_qkv': w_qkv, 'w_out': w_out, 'w_up': w_up, 'w_down': w_down}


def reference(x, norm_gain, norm_shift, w_qkv, w_out, w_up, w_down):
    num_videos, num_frames, num_patches, model_width = x.shape

    def spatial_fn(frame_tok):
        return seq_block(frame_tok, norm_gain[0], norm_shift[0], w_qkv[0], w_out[0], w_up[0], w_down[0])

    def temporal_fn(tube_tok):
        return seq_block(tube_tok, norm_gain[1], norm_shift[1], w_qkv[1], w_out[1], w_up[1], w_down[1])

    frame_rows = x.reshape(num_videos * num_frames, num_patches, model_width)
    spatial_out = lax.map(spatial_fn, frame_rows).reshape(num_videos, num_frames, num_patches, model_width)
    tube_rows = jnp.transpose(spatial_out, (0, 2, 1, 3)).reshape(num_videos * num_patches, num_frames, model_width)
    temporal_out = lax.map(temporal_fn, tube_rows).reshape(num_videos, num_patches, num_frames, model_width)
    return jnp.transpose(temporal_out, (0, 2, 1, 3))
```

```python
import functools
import math

import jax
import jax.numpy as jnp
from jax import lax
from jax.experimental import pallas as pl
from jax.experimental.pallas import tpu as pltpu
from jax.sharding import PartitionSpec as P

LN_EPS = 1e-6
HEADS = 16
HEAD = 72
ROWS = 80
WIDTH = HEADS * HEAD
WIDE = HEADS * ROWS
FF = 4 * WIDTH
SPATIAL_HEADS, TEMPORAL_HEADS = 8, 8
SOFTMAX_SCALE = (HEAD ** -0.5) * math.log2(math.e)
VMEM_LIMIT = 60 * 1024 * 1024
F32 = jnp.float32
BF16 = jnp.bfloat16


def layer_norm(tokens, gain, shift):
    tok = tokens.astype(F32)
    centered = tok - jnp.mean(tok, axis=-1, keepdims=True)
    var = jnp.mean(centered * centered, axis=-1, keepdims=True)
    normed = centered * lax.rsqrt(var + LN_EPS)
    return (normed * gain.astype(F32) + shift.astype(F32)).astype(BF16)


def project_qkv(n_s, w_ref, qkv_s, length, stride):
    for j in range(3):
        rows = pl.ds(j * WIDE, WIDE)
        proj = lax.dot_general(
            w_ref[rows, :], n_s[...], (((1,), (1,)), ((), ())), preferred_element_type=F32
        ).astype(BF16)
        if length == stride:
            qkv_s[rows, :] = proj
        else:
            for p in range(proj.shape[1] // length):
                qkv_s[rows, pl.ds(p * stride, length)] = proj[:, p * length:(p + 1) * length]


def attend_all(qkv_s, o_s, sequences, length, stride, heads):
    def refs(head, seq):
        row = pl.multiple_of(head * ROWS, 16)
        return row, pl.ds(seq * stride, length)

    def per_step(step, carry):
        units = [(step * heads + i, seq) for i in range(heads) for seq in range(sequences)]
        scores = []
        for head, seq in units:
            row, cols = refs(head, seq)
            q = qkv_s[pl.ds(row, ROWS), cols]
            k = qkv_s[pl.ds(WIDE + row, ROWS), cols]
            scores.append(lax.dot_general(k, q, (((0,), (0,)), ((), ())), preferred_element_type=F32))
        probs = []
        for s in scores:
            e = jnp.exp2((s - jnp.max(s, axis=0, keepdims=True)) * SOFTMAX_SCALE)
            probs.append((e * (1.0 / jnp.sum(e, axis=0, keepdims=True))).astype(BF16))
        for (head, seq), p in zip(units, probs):
            row, cols = refs(head, seq)
            v = qkv_s[pl.ds(2 * WIDE + row, ROWS), cols]
            o = jnp.dot(v, p, preferred_element_type=F32)
            o_s[pl.ds(row, ROWS), pl.ds(seq * length, length)] = o.astype(BF16)
        return carry

    lax.fori_loop(0, HEADS // heads, per_step, 0)


def project_out(o_s, w_ref):
    return lax.dot_general(o_s[...], w_ref[...], (((0,), (0,)), ((), ())), preferred_element_type=F32).astype(BF16)


def spatial_kernel(x_ref, gain_ref, shift_ref, wqkv_ref, wout_ref, h_ref, n_s, qkv_s, o_s):
    frames, patches, width = h_ref.shape
    tok = frames * patches
    n_s[...] = layer_norm(x_ref[0].reshape(tok, width), gain_ref[...], shift_ref[...])
    project_qkv(n_s, wqkv_ref, qkv_s, patches, patches)

    attend_all(qkv_s, o_s, frames, patches, patches, SPATIAL_HEADS)
    a = project_out(o_s, wout_ref)
    h = x_ref[0].reshape(tok, width).astype(F32) + a.astype(F32)
    h_ref[...] = h.astype(BF16).reshape(frames, patches, width)


def temporal_kernel(stride, x_ref, gain_ref, shift_ref, wqkv_ref, wout_ref, h_ref, n_s, qkv_s, o_s, a_s):
    groups, patches, frames, width = x_ref.shape
    length = groups * frames
    for p in range(patches):
        for g in range(groups):
            n_s[pl.ds(p * length + g * frames, frames), :] = layer_norm(x_ref[g, p], gain_ref[...], shift_ref[...])
    project_qkv(n_s, wqkv_ref, qkv_s, length, stride)

    attend_all(qkv_s, o_s, patches, length, stride, TEMPORAL_HEADS)
    a_s[...] = project_out(o_s, wout_ref)
    for p in range(patches):
        for g in range(groups):
            a = a_s[pl.ds(p * length + g * frames, frames), :]
            h_ref[g, p] = (x_ref[g, p].astype(F32) + a.astype(F32)).astype(BF16)


def mlp_kernel(chunk, h_ref, gain_ref, shift_ref, up_ref, down_ref, *rest):
    y_ref, n_s, acc_s = rest[-3:]
    h = h_ref[...]
    n_s[...] = layer_norm(h, gain_ref[...], shift_ref[...])
    for c in range(0, FF, chunk):
        u = jnp.dot(n_s[...], up_ref[:, c:c + chunk], preferred_element_type=F32).astype(BF16)
        g = jax.nn.gelu(u.astype(F32), approximate=True).astype(BF16)
        part = jnp.dot(g, down_ref[c:c + chunk, :], preferred_element_type=F32)
        if c == 0:
            acc_s[...] = part
        elif c + chunk < FF:
            acc_s[...] += part
        else:
            m = (acc_s[...] + part).astype(BF16)
            y_ref[...] = (h.astype(F32) + m.astype(F32)).astype(BF16).reshape(y_ref.shape)


def pick(array, *at):
    rest = array.shape[len(at):]
    return pl.BlockSpec((None,) * len(at) + rest, lambda i: at + (0,) * len(rest), pipeline_mode=pl.Buffered(1))


def params():
    return pltpu.CompilerParams(dimension_semantics=("arbitrary",), vmem_limit_bytes=VMEM_LIMIT)


def attention_cost(tokens, keys):
    return pl.CostEstimate(
        flops=2 * tokens * WIDTH * (4 * WIDTH + 2 * keys), bytes_accessed=4 * tokens * WIDTH, transcendentals=tokens * keys * HEADS
    )


def spatial_attention(x, video, gain, shift, wqkv, wout, frames=4):
    _, num_frames, patches, width = x.shape
    tok = frames * patches
    return pl.pallas_call(
        spatial_kernel,
        name="spatial_attention",
        grid=(num_frames // frames,),
        in_specs=[
            pl.BlockSpec((1, frames, patches, width), lambda i: (video, i, 0, 0)),
            pick(gain, 0, 0), pick(shift, 0, 0), pick(wqkv, 0), pick(wout, 0),
        ],
        out_specs=pl.BlockSpec((frames, patches, width), lambda i: (i, 0, 0)),
        out_shape=jax.ShapeDtypeStruct((num_frames, patches, width), BF16),
        scratch_shapes=[
            pltpu.VMEM((tok, width), BF16), pltpu.VMEM((3 * WIDE, tok), BF16), pltpu.VMEM((WIDE, tok), BF16),
        ],
        compiler_params=params(),
        cost_estimate=attention_cost(num_frames * patches, patches),
    )(x, gain, shift, wqkv, wout)


def temporal_attention(x, gain, shift, wqkv, wout, patches=4):
    groups, num_patches, frames, width = x.shape
    length = groups * frames
    stride = -(-length // 128) * 128
    tok = patches * length
    spec = pl.BlockSpec((groups, patches, frames, width), lambda i: (0, i, 0, 0))
    return pl.pallas_call(
        functools.partial(temporal_kernel, stride),
        name="temporal_attention",
        grid=(num_patches // patches,),
        in_specs=[spec, pick(gain, 1, 0), pick(shift, 1, 0), pick(wqkv, 1), pick(wout, 1)],
        out_specs=spec,
        out_shape=jax.ShapeDtypeStruct(x.shape, BF16),
        scratch_shapes=[
            pltpu.VMEM((tok, width), BF16), pltpu.VMEM((3 * WIDE, patches * stride), BF16), pltpu.VMEM((WIDE, tok), BF16),
            pltpu.VMEM((tok, width), BF16),
        ],
        compiler_params=params(),
        cost_estimate=attention_cost(num_patches * length, length),
    )(x, gain, shift, wqkv, wout)


def mlp(h, block, gain, shift, w_up, w_down, videos=None, video=0, into=None, tok=512, chunk=1536):
    tokens, width = h.shape
    in_specs = [
        pl.BlockSpec((tok, width), lambda i: (i, 0)),
        pick(gain, block, 1), pick(shift, block, 1), pick(w_up, block), pick(w_down, block),
    ]
    args = [h, gain, shift, w_up, w_down]
    aliases = {}
    if videos is None:
        out_spec = pl.BlockSpec((tok, width), lambda i: (i, 0))
        out_shape = jax.ShapeDtypeStruct((tokens, width), BF16)
    else:
        out_spec = pl.BlockSpec((1, tok, width), lambda i: (video, i, 0))
        out_shape = jax.ShapeDtypeStruct((videos, tokens, width), BF16)
    if into is not None:
        in_specs.append(pl.BlockSpec(memory_space=pl.ANY))
        args.append(into)
        aliases = {len(args) - 1: 0}
    return pl.pallas_call(
        functools.partial(mlp_kernel, chunk),
        name="mlp",
        grid=(tokens // tok,),
        in_specs=in_specs,
        out_specs=out_spec,
        out_shape=out_shape,
        scratch_shapes=[pltpu.VMEM((tok, width), BF16), pltpu.VMEM((tok, width), F32)],
        input_output_aliases=aliases,
        compiler_params=params(),
        cost_estimate=pl.CostEstimate(
            flops=4 * tokens * width * FF, bytes_accessed=4 * tokens * width + 4 * width * FF, transcendentals=tokens * FF
        ),
    )(*args)


def pad_heads(w_qkv, w_out):
    pad = ROWS - HEAD
    wqkv = jnp.pad(jnp.transpose(w_qkv, (0, 1, 3, 4, 2)), ((0, 0), (0, 0), (0, 0), (0, pad), (0, 0)))
    wout = jnp.pad(w_out, ((0, 0), (0, 0), (0, pad), (0, 0)))
    return wqkv.reshape(-1, 3 * WIDE, WIDTH), wout.reshape(-1, WIDE, WIDTH)


def solution(mesh):
    tok_spec = P(('pod', 'dp'), 'sp', None, None)
    sp = mesh.shape['sp']

    def local_step(x, norm_gain, norm_shift, w_qkv, w_out, w_up, w_down):
        videos, frames, patches, width = x.shape
        gain, shift = norm_gain[:, :, None, :], norm_shift[:, :, None, :]
        wqkv, wout = pad_heads(w_qkv, w_out)

        sent = []
        for v in range(videos):
            h = spatial_attention(x, v, gain, shift, wqkv, wout)
            t = mlp(h.reshape(frames * patches, width), 0, gain, shift, w_up, w_down)
            t = jnp.transpose(t.reshape(frames, patches, width), (1, 0, 2)).reshape(sp, patches // sp, frames, width)
            sent.append(lax.all_to_all(t, 'sp', 0, 0, tiled=True))
        back = []
        for v in range(videos):
            h = temporal_attention(sent[v], gain, shift, wqkv, wout)
            back.append(lax.all_to_all(h, 'sp', 0, 0, tiled=True))
        y = None
        for v in range(videos):
            if v:
                back[v], y = lax.optimization_barrier((back[v], y))
            h = jnp.transpose(back[v].reshape(patches, frames, width), (1, 0, 2)).reshape(frames * patches, width)
            y = mlp(h, 1, gain, shift, w_up, w_down, videos, v, y)
        return y.reshape(videos, frames, patches, width)

    return jax.shard_map(
        local_step, mesh=mesh, in_specs=(tok_spec, P(), P(), P(), P(), P(), P()), out_specs=tok_spec, check_vma=False
    )
```
